256 devices in a mesh: grp: 2 (over y), row: 128 (over x, z, core).
Axes of the slice: x: 4, y: 2, z: 16, core: 2. Of those that a mesh axis runs over, the one named last changes fastest.
The devices are a block of a 4x16x16 slice.
Arguments:
- sensing: float32 [24576, 16384], P('row')
- measured: float32 [12288], P(('grp', 'row')), parts along dimension 0, may hold values from -6 to 6
- thresholds: float32 [12], P('grp'), parts along dimension 0, may hold values from 3 to 4
Outputs:
- estimate: float32 [131072], P(('grp', 'row')), parts along dimension 0
- residual: float32 [12288], P(('grp', 'row')), parts along dimension 0
The draws below stay inside these ranges and needn't reach their ends.
There are 2 independent parts, one for each index of `grp`. The reference program is written for one: setup_inputs(seed, part) draws one part's arguments, and reference() takes and returns one part's arrays. A program takes and returns all parts, laid end to end along the dimension named above; an argument that names none is the same for every part. Nothing has to cross between parts.
All inputs are finite; a program needn't handle non-finite values.
Results may differ from the reference program's by a relative error of at most 0.0003.
Values sent between devices are 32-bit elements; how exact they have to be, the bound alone decides.
A program may use at most 64 MiB of HBM per device.

```python
import math
import jax
import jax.numpy as jnp
from jax import lax

N = 65536
COLS = 4
ROWS_DEV = 48
ITERS = 6
M = 6144
N_ROW = 128


def draw_sensing(key, part):
    positions = jnp.arange(N, dtype=jnp.float32) / N
    entries = jax.random.normal(jax.random.fold_in(key, 13), (M, N), jnp.float32)
    jitter = jax.random.uniform(jax.random.fold_in(key, 14), (N,), jnp.float32, 0.8, 1.25)
    column_scale = 0.5 * jnp.exp(positions * math.log(3.0)) * jitter
    matrix = entries * column_scale[None, :] / math.sqrt(M)
    groups = M // ROWS_DEV // COLS
    width = N // COLS
    blocks = matrix.reshape(COLS, groups, ROWS_DEV, COLS, width).transpose(3, 1, 0, 2, 4)
    return blocks.reshape(M * COLS, width)


def levels(stream_key, dims, split, low, high):
    gain = 1.0
    for axis_at, shards_of in split:
        draws = jax.random.uniform(jax.random.fold_in(jax.random.fold_in(stream_key, 6), axis_at), (shards_of,), jnp.float32, low / len(split), high / len(split))
        gain = gain * jnp.repeat(jnp.exp(draws), dims[axis_at] // shards_of).reshape((-1,) + (1,) * (len(dims) - 1 - axis_at))
    return gain


def bell_draw(stream_key, shape, scale, limit, split=(), kind=jnp.bfloat16):
    values = scale * jax.random.normal(stream_key, shape, jnp.float32)
    if split:
        values = values * levels(stream_key, shape, split, -0.22, 0.18)
    return jnp.clip(values, -limit, limit).astype(kind)


def setup_inputs(seed: int = 0, part: int = 0) -> dict:
    streams_of = jax.random.split(jax.random.key(seed), 4)
    part_splits = jax.random.split(jax.random.fold_in(streams_of[3], part), 4)
    sensing = draw_sensing(jax.random.fold_in(streams_of[3], 71), part)
    measured = bell_draw(part_splits[1], (M,), 1.0, 6.0, ((0, 128),), jnp.float32)
    thresholds = jnp.clip(jax.random.uniform(part_splits[2], (ITERS,), jnp.float32, 3.0, 4.0), 3.0, 4.0)
    return dict(sensing=sensing, measured=measured, thresholds=thresholds)


SOFTNESS = 0.25


def shrink(values, level):
    return SOFTNESS * (jax.nn.softplus((values - level) / SOFTNESS) - jax.nn.softplus((-values - level) / SOFTNESS))


def slopes(values, level):
    return jax.nn.sigmoid((values - level) / SOFTNESS) + jax.nn.sigmoid((-values - level) / SOFTNESS)


def reference(sensing, measured, thresholds):
    groups = N_ROW // COLS
    width = N // COLS
    matrix = sensing.reshape(COLS, groups, COLS, ROWS_DEV, width).transpose(2, 1, 3, 0, 4).reshape(M, N)
    estimate = jnp.zeros((N,), jnp.float32)
    residual = measured
    for step in range(ITERS):
        pseudo = estimate + jnp.dot(residual, matrix, precision=lax.Precision.HIGHEST, preferred_element_type=jnp.float32)
        onsager = jnp.sum(slopes(pseudo, thresholds[step])) / M
        estimate = shrink(pseudo, thresholds[step])
        product = jnp.dot(matrix, estimate, precision=lax.Precision.HIGHEST, preferred_element_type=jnp.float32)
        residual = measured - product + onsager * residual
    return estimate, residual
```

```python
import functools

import jax
import jax.numpy as jnp
from jax import lax
from jax.experimental import pallas as pl
from jax.experimental.pallas import tpu as pltpu
from jax.sharding import PartitionSpec as P

COLS = 4
CORES = 2
ITERS = 6
SOFTNESS = 0.25
LANES = 128
SUBLANES = 8
MESH = pl.DeviceIdType.MESH


def ring_plan(chips):
    quarter = chips // 4
    half = chips // 2
    near = [0] + [d for k in range(1, quarter) for d in (k, -k)] + [quarter]
    window = sorted((d for d in near if d), key=lambda d: -abs(d))
    centre = quarter
    spread = sorted(
        range(centre - quarter // 2, centre + quarter // 2),
        key=lambda e: max(e, half - e),
    )
    return quarter, half, window, spread


def shrink_and_slope(values, level):
    up = (values - level) / SOFTNESS
    down = (-values - level) / SOFTNESS
    up_tail = jnp.exp(-jnp.abs(up))
    down_tail = jnp.exp(-jnp.abs(down))
    one_up = 1.0 + up_tail
    one_down = 1.0 + down_tail
    shrunk = SOFTNESS * (
        jnp.maximum(up, 0.0)
        - jnp.maximum(down, 0.0)
        + jnp.log1p((up_tail - down_tail) / one_down)
    )
    slope = jnp.where(up >= 0, 1.0, up_tail) / one_up + jnp.where(down >= 0, 1.0, down_tail) / one_down
    return shrunk, slope


def kernel(
    devices,
    measurements,
    thresholds,
    measured,
    sensing_hbm,
    estimate_out,
    residual_out,
    sensing,
    partial,
    partner_partial,
    window_in,
    half_sum,
    spread_in,
    pseudo,
    estimate,
    row_send,
    row_in,
    measured_tile,
    residual_tile,
    residual_wide,
    load_sem,
    pair_send,
    pair_recv,
    back_send,
    back_recv,
    window_send,
    window_recv,
    spread_send,
    spread_recv,
    row_send_sem,
    row_recv_sem,
):
    chips = devices // (COLS * CORES)
    quarter, half, window, spread = ring_plan(chips)
    rows = sensing.shape[0]
    width = sensing.shape[1]
    groups = rows // SUBLANES
    lines = width // LANES
    part_lines = lines // quarter
    core_lines = part_lines // CORES
    part_width = width // quarter
    own_groups = groups // COLS
    block_width = SUBLANES * LANES

    me = lax.axis_index("row")
    core = me % CORES
    z = (me // CORES) % chips
    x = me // (CORES * chips)

    def place(dx, dz, other=False):
        at = ((x + dx + COLS) % COLS) * chips + (z + dz + chips) % chips
        return {"row": at * CORES + (1 - core if other else core)}

    def part_of(offset):
        return (z + offset + chips) % quarter

    def core_rows(part, owner):
        return pl.ds(pl.multiple_of(part * part_lines + owner * core_lines, core_lines), core_lines)

    order = [d % quarter for d in (quarter, 1, quarter - 1)]
    order = order + [d for d in range(quarter) if d not in order]

    loads = []
    for at, offset in enumerate(order):
        columns = pl.ds(pl.multiple_of(part_of(offset) * part_width, part_width), part_width)
        load = pltpu.make_async_copy(sensing_hbm.at[:, columns], sensing.at[:, columns], load_sem.at[at])
        load.start()
        loads.append(load)

    reach = set()
    for d in window + [-e for e in spread] + [half - e for e in spread]:
        reach |= {d, -d}
    greeted = [place(dx, 0) for dx in range(1, COLS)] + [place(0, 0, True)]
    greeted = greeted + [place(0, d) for d in sorted(reach)]
    barrier = pltpu.get_barrier_semaphore()
    for device in greeted:
        pl.semaphore_signal(barrier, inc=1, device_id=device, device_id_type=MESH)
    pl.semaphore_wait(barrier, len(greeted))

    lane = lax.broadcasted_iota(jnp.int32, (SUBLANES, LANES), 1)
    sublane = lax.broadcasted_iota(jnp.int32, (SUBLANES, LANES), 0)

    def row_sum(tile, slot):
        row_send[slot] = tile
        copies = []
        for at, dx in enumerate((2, 1, 3)):
            copy = pltpu.make_async_remote_copy(
                src_ref=row_send.at[slot],
                dst_ref=row_in.at[slot, at],
                send_sem=row_send_sem.at[slot, at],
                recv_sem=row_recv_sem.at[slot, at],
                device_id=place(dx, 0),
                device_id_type=MESH,
            )
            copy.start()
            copies.append(copy)
        total = tile
        for at in (1, 2, 0):
            copies[at].wait()
            total = total + row_in[slot, at]
        return total

    def widen(tile):
        residual_tile[...] = tile
        for k in range(groups):
            residual_wide[pl.ds(k * SUBLANES, SUBLANES), :] = jnp.broadcast_to(
                tile[:, k : k + 1], (SUBLANES, LANES)
            )

    line = jnp.concatenate(
        [measured[...], jnp.zeros((1, LANES - measured.shape[1]), jnp.float32)], axis=1
    )
    line = jnp.broadcast_to(line, (SUBLANES, LANES))
    tile = jnp.zeros((SUBLANES, LANES), jnp.float32)
    for g in range(own_groups):
        value = jnp.sum(jnp.where(lane == g * SUBLANES + sublane, line, 0.0), axis=1, keepdims=True)
        tile = tile + jnp.where(lane == x * own_groups + g, value, 0.0)
    tile = row_sum(tile, 0)
    measured_tile[...] = tile
    widen(tile)
    estimate[...] = jnp.zeros_like(estimate)
    for load in loads:
        load.wait()

    def back_project(part, owner):
        start = part * part_lines + owner * core_lines

        def body(g, carry):
            first = pl.multiple_of(start + g * SUBLANES, SUBLANES)
            columns = pl.ds(pl.multiple_of(first * LANES, block_width), block_width)
            total = jnp.zeros((SUBLANES, block_width), jnp.float32)
            for k in range(groups):
                span = pl.ds(k * SUBLANES, SUBLANES)
                wide = residual_wide[span, :]
                total = total + sensing[span, columns] * jnp.concatenate([wide] * SUBLANES, axis=1)
            block = jnp.zeros((SUBLANES, LANES), jnp.float32)
            for j in range(SUBLANES):
                piece = total[:, j * LANES : (j + 1) * LANES]
                for shift in (4, 2, 1):
                    piece = piece + pltpu.roll(piece, shift, 0)
                block = jnp.where(sublane == j, piece, block)
            partial[pl.ds(first, SUBLANES), :] = block
            return carry

        lax.fori_loop(0, core_lines // SUBLANES, body, 0)

    def project(part, owner, sums):
        start = part * part_lines + owner * core_lines

        def body(g, sums):
            first = pl.multiple_of(start + g * SUBLANES, SUBLANES)
            columns = pl.ds(pl.multiple_of(first * LANES, block_width), block_width)
            spread_lines = jnp.concatenate(
                [
                    jnp.broadcast_to(estimate[pl.ds(first + j, 1), :], (SUBLANES, LANES))
                    for j in range(SUBLANES)
                ],
                axis=1,
            )
            result = []
            for k in range(groups):
                product = sensing[pl.ds(k * SUBLANES, SUBLANES), columns] * spread_lines
                total = sums[k]
                for j in range(SUBLANES):
                    total = total + product[:, j * LANES : (j + 1) * LANES]
                result.append(total)
            return tuple(result)

        return lax.fori_loop(0, core_lines // SUBLANES, body, sums)

    def pair_copy(at):
        span = core_rows(part_of(order[at]), 1 - core)
        return pltpu.make_async_remote_copy(
            src_ref=partial.at[span, :],
            dst_ref=partner_partial.at[span, :],
            send_sem=pair_send.at[at],
            recv_sem=pair_recv.at[at],
            device_id=place(0, 0, True),
            device_id_type=MESH,
        )

    def back_copy(at):
        span = core_rows(part_of(spread[at]), core)
        return pltpu.make_async_remote_copy(
            src_ref=pseudo.at[span, :],
            dst_ref=pseudo.at[span, :],
            send_sem=back_send.at[at],
            recv_sem=back_recv.at[at],
            device_id=place(0, 0, True),
            device_id_type=MESH,
        )

    def window_copy(at, slot):
        return pltpu.make_async_remote_copy(
            src_ref=partial.at[core_rows(part_of(window[at]), core), :],
            dst_ref=window_in.at[slot, at],
            send_sem=window_send.at[at],
            recv_sem=window_recv.at[slot, at],
            device_id=place(0, window[at]),
            device_id_type=MESH,
        )

    sides = [(e, side) for e in spread for side in (0, 1)]

    def spread_distance(at):
        e, side = sides[at]
        return half - e if side else -e

    def spread_copy(at, slot):
        return pltpu.make_async_remote_copy(
            src_ref=half_sum,
            dst_ref=spread_in.at[slot, at],
            send_sem=spread_send.at[at],
            recv_sem=spread_recv.at[slot, at],
            device_id=place(0, spread_distance(at)),
            device_id_type=MESH,
        )

    def iteration(step, carry):
        slot = step % 2
        level = thresholds[step]

        for at, offset in enumerate(order):
            back_project(part_of(offset), 1 - core)
            pair_copy(at).start()
        for offset in order:
            back_project(part_of(offset), core)

        for at, offset in enumerate(order):
            pair_copy(at).wait_recv()
            span = core_rows(part_of(offset), core)
            partial[span, :] = partial[span, :] + partner_partial[span, :]
            for index, d in enumerate(window):
                if d % quarter == offset:
                    window_copy(index, slot).start()
        total = partial[core_rows(part_of(0), core), :]
        for index in reversed(range(len(window))):
            window_copy(index, slot).wait_recv()
            total = total + window_in[slot, index]
        half_sum[...] = total
        for index in sorted(range(len(sides)), key=lambda at: -abs(spread_distance(at))):
            spread_copy(index, slot).start()

        sums = tuple(jnp.zeros((SUBLANES, LANES), jnp.float32) for _ in range(groups))
        slopes = jnp.zeros((SUBLANES, LANES), jnp.float32)

        def advance(part, owner, sums, slopes):
            span = core_rows(part, owner)
            shrunk, slope = shrink_and_slope(pseudo[span, :], level)
            estimate[span, :] = shrunk
            for g in range(core_lines // SUBLANES):
                slopes = slopes + slope[g * SUBLANES : (g + 1) * SUBLANES, :]
            return project(part, owner, sums), slopes

        for at, e in enumerate(spread):
            span = core_rows(part_of(e), core)
            for side in (0, 1):
                spread_copy(2 * at + side, slot).wait_recv()
            pseudo[span, :] = estimate[span, :] + (
                spread_in[slot, 2 * at] + spread_in[slot, 2 * at + 1]
            )
            back_copy(at).start()
            sums, slopes = advance(part_of(e), core, sums, slopes)
        for at, e in enumerate(spread):
            back_copy(at).wait_recv()
            sums, slopes = advance(part_of(e), 1 - core, sums, slopes)

        tile = jnp.where(lane == groups, jnp.sum(slopes, axis=1, keepdims=True), 0.0)
        for k in range(groups):
            piece = jnp.sum(sums[k], axis=1, keepdims=True)
            tile = jnp.where(lane == k, piece, tile)
        tile = row_sum(tile, (step + 1) % 2)
        onsager = jnp.sum(jnp.where(lane == groups, tile, 0.0), axis=(0, 1), keepdims=True) / measurements
        product = jnp.where(lane < groups, tile, 0.0)
        widen(measured_tile[...] - product + onsager * residual_tile[...])

        for at in range(quarter):
            pair_copy(at).wait_send()
            back_copy(at).wait_send()
        for at in range(len(window)):
            window_copy(at, slot).wait_send()
        for at in range(len(sides)):
            spread_copy(at, slot).wait_send()

        return carry

    lax.fori_loop(0, ITERS, iteration, 0)

    own_lines = lines // (chips * CORES)
    estimate_out[...] = estimate[pl.ds((z * CORES + core) * own_lines, own_lines), :]
    picked = jnp.zeros((SUBLANES, LANES), jnp.float32)
    for g in range(own_groups):
        at = pl.multiple_of((x * own_groups + g) * SUBLANES, SUBLANES)
        picked = jnp.where(lane == g * SUBLANES + sublane, residual_wide[pl.ds(at, SUBLANES), :], picked)
    residual_out[...] = jnp.sum(picked, axis=0, keepdims=True)[:, : residual_out.shape[1]]


def solution(mesh):
    devices = mesh.shape["row"]
    chips = devices // (COLS * CORES)
    quarter, half, window, spread = ring_plan(chips)

    def on_device(sensing, measured, thresholds):
        rows, width = sensing.shape
        local_rows = measured.shape[0]
        lines = width // LANES
        core_lines = lines // quarter // CORES
        own_lines = lines // (chips * CORES)
        vmem = pl.BlockSpec(memory_space=pltpu.VMEM)
        f32 = jnp.float32
        estimate, residual = pl.pallas_call(
            functools.partial(kernel, devices, float(local_rows * devices)),
            out_shape=(
                jax.ShapeDtypeStruct((own_lines, LANES), f32),
                jax.ShapeDtypeStruct((1, local_rows), f32),
            ),
            in_specs=[
                pl.BlockSpec(memory_space=pltpu.SMEM),
                vmem,
                pl.BlockSpec(memory_space=pl.ANY),
            ],
            out_specs=(vmem, vmem),
            scratch_shapes=[
                pltpu.VMEM((rows, width), f32),
                pltpu.VMEM((lines, LANES), f32),
                pltpu.VMEM((lines, LANES), f32),
                pltpu.VMEM((2, len(window), core_lines, LANES), f32),
                pltpu.VMEM((core_lines, LANES), f32),
                pltpu.VMEM((2, 2 * len(spread), core_lines, LANES), f32),
                pltpu.VMEM((lines, LANES), f32),
                pltpu.VMEM((lines, LANES), f32),
                pltpu.VMEM((2, SUBLANES, LANES), f32),
                pltpu.VMEM((2, COLS - 1, SUBLANES, LANES), f32),
                pltpu.VMEM((SUBLANES, LANES), f32),
                pltpu.VMEM((SUBLANES, LANES), f32),
                pltpu.VMEM((rows, LANES), f32),
                pltpu.SemaphoreType.DMA((quarter,)),
                pltpu.SemaphoreType.DMA((quarter,)),
                pltpu.SemaphoreType.DMA((quarter,)),
                pltpu.SemaphoreType.DMA((quarter,)),
                pltpu.SemaphoreType.DMA((quarter,)),
                pltpu.SemaphoreType.DMA((len(window),)),
                pltpu.SemaphoreType.DMA((2, len(window))),
                pltpu.SemaphoreType.DMA((2 * len(spread),)),
                pltpu.SemaphoreType.DMA((2, 2 * len(spread))),
                pltpu.SemaphoreType.DMA((2, COLS - 1)),
                pltpu.SemaphoreType.DMA((2, COLS - 1)),
            ],
            compiler_params=pltpu.CompilerParams(
                collective_id=0, has_side_effects=True, vmem_limit_bytes=63 * 1024 * 1024
            ),
            name="amp",
        )(thresholds, measured.reshape(1, local_rows), sensing)
        return estimate.reshape(-1), residual.reshape(-1)

    return jax.shard_map(
        on_device,
        mesh=mesh,
        in_specs=(P("row", None), P(("grp", "row")), P("grp")),
        out_specs=(P(("grp", "row")), P(("grp", "row"))),
        check_vma=False,
    )
```
